32 devices in a mesh: band: 4 (over y, core), tile: 8 (over z, x).
Axes of the slice: x: 2, y: 2, z: 4, core: 2. Of those that a mesh axis runs over, the one named last changes fastest.
Arguments:
- patches: bfloat16 [262144, 128], P(('band', 'tile')), may hold values from -6 to 6
- pair_patch: int32 [4096], P(('band', 'tile')), may hold values from 0 to 63
- pair_atm: int32 [4096], P(('band', 'tile')), may hold values from 0 to 4095, as said below
- numerators: int32 [4096, 128, 32], P(('band', 'tile')), may hold values from 0 to 16777215
- counts: int32 [32], P(('band', 'tile')), may hold values from 32 to 128, as said below
Outputs:
- atmosphere: float32 [131072, 128], P(('band', 'tile'))
The draws below stay inside these ranges and needn't reach their ends.
Inputs may be any that keep to these rules, and one draw needn't show every extreme that they name: Block pair_atm[g] is owned by device pair_atm[g] // 128 (band-major device order). Every live pair of device (b, t) targets an owner in band b (any tile) or one of (b - 1, t), (b + 1, t). Among one device's live pairs at most 32 target one owner and at most 16 distinct blocks of one owner; both are reached on some device in every draw. Slots that are not live hold arbitrary blocks in range. `counts`: the value 128 occurs on some device in every draw.
All inputs are finite; a program needn't handle non-finite values.
Results may differ from the reference program's by a relative error of at most 0.0026.
Values sent between devices are 32-bit elements; how exact they have to be, the bound alone decides.
No kernel may reach another device: no remote copies, remote signals or barrier semaphores. Data moves between devices by JAX's collectives and lax.ppermute only.
A program may use at most 64 MiB of HBM per device.

```python
import jax
import jax.numpy as jnp
from jax import lax

FLUX = 128
PATCH_BLK = 128
CELL_BLK = 32
PBLK_DEV = 64
CELLS_DEV = 4096
PATCHES = 262144
ALL_PAIRS = 4096
N_BAND = 4
N_TILE = 8


def shuffle_one(subkey):
    return jax.random.permutation(subkey, 2 * PBLK_DEV)


def routing(key):
    base_key = jax.random.fold_in(key, 7)
    subkeys = jax.random.split(base_key, 7)
    devices_all = N_BAND * N_TILE
    pairs_here = 2 * PBLK_DEV
    capacity = PBLK_DEV // 2
    distinct = capacity // 2
    blocks_owned = CELLS_DEV // CELL_BLK
    window = blocks_owned // distinct
    device_ids = jnp.arange(devices_all)
    band_of = (device_ids // N_TILE)[:, None]
    tile_of = (device_ids % N_TILE)[:, None]
    fullest_band = jax.random.randint(subkeys[4], (), 1, N_BAND - 1)
    fullest_tile = jax.random.randint(subkeys[5], (), 0, N_TILE)
    fullest = fullest_band * N_TILE + fullest_tile
    offset_far = jax.random.randint(subkeys[6], (devices_all, 1), 1, N_TILE)
    offset_far = jnp.where(device_ids[:, None] == fullest, N_TILE // 2, offset_far)
    offset_edge = jnp.where(offset_far == N_TILE - 1, 1, offset_far + 1)
    position = jnp.arange(pairs_here)[None, :]
    group = jnp.broadcast_to(position // capacity, (devices_all, pairs_here))
    candidate = jnp.broadcast_to(position % distinct, (devices_all, pairs_here))
    target_band = band_of + jnp.where(group == 1, -1, jnp.where(group == 2, 1, 0))
    target_tile = tile_of + jnp.where(group == 0, offset_far, 0)
    low_edge = (group == 1) & (band_of == 0)
    high_edge = (group == 2) & (band_of == N_BAND - 1)
    at_edge = low_edge | high_edge
    target_band = jnp.where(at_edge, band_of, target_band)
    target_tile = jnp.where(at_edge, tile_of + offset_edge, target_tile) % N_TILE
    owner = target_band * N_TILE + target_tile
    anchor = jax.random.randint(subkeys[0], (devices_all, 4), 0, blocks_owned)
    offsets = jax.random.randint(subkeys[1], (devices_all, 4 * distinct), 0, window)
    anchor_pick = jnp.take_along_axis(anchor, group, axis=1)
    offset_pick = jnp.take_along_axis(offsets, group * distinct + candidate, axis=1)
    local_block = (anchor_pick + candidate * window + offset_pick) % blocks_owned
    global_block = owner * blocks_owned + local_block
    shuffles = jax.vmap(shuffle_one)(jax.random.split(subkeys[2], devices_all))
    global_block = jnp.take_along_axis(global_block, shuffles, axis=1)
    live_counts = jax.random.randint(subkeys[3], (devices_all,), pairs_here // 4, pairs_here + 1)
    live_counts = jnp.where(device_ids == fullest, pairs_here, live_counts)
    return (global_block.reshape(-1).astype(jnp.int32), live_counts.astype(jnp.int32))


def draw_pair_atm(key, part):
    return routing(key)[0]


def draw_counts(key, part):
    return routing(key)[1]


def touch_ends(values, stream_key, least, high):
    extent = values.shape
    index_at = [jax.random.randint(jax.random.fold_in(stream_key, axis), (), 0, extent[axis]) for axis in range(len(extent))]
    values = values.at[tuple(index_at)].set(least)
    longest = extent.index(max(extent))
    index_at[longest] = (index_at[longest] + 1) % extent[longest]
    return values.at[tuple(index_at)].set(high)


def steps_of(stream_key, dims, cuts, smallest, top_value):
    level, own = 1.0, jax.random.fold_in(stream_key, 6)
    for dim, blocks in cuts:
        steps = jnp.exp(jax.random.uniform(jax.random.fold_in(own, dim), (blocks,), jnp.float32, smallest / len(cuts), top_value / len(cuts)))
        level = level * jnp.repeat(steps, dims[dim] // blocks).reshape([-1 if axis == dim else 1 for axis in range(len(dims))])
    return level


def noise(own_key, shape, width, most, shards=(), held_as=jnp.bfloat16):
    loudness = steps_of(own_key, shape, shards, -0.22, 0.18) if shards else 1.0
    result = jax.random.normal(own_key, shape, jnp.float32) * width * loudness
    return jnp.minimum(jnp.maximum(result, -most), most).astype(held_as)


def setup_inputs(seed: int = 0) -> dict:
    key_list = jax.random.split(jax.random.key(seed), 6)
    return {
        "patches": noise(key_list[0], (PATCHES, FLUX), 1.0, 6.0, ((0, 32),)),
        "pair_patch": touch_ends(jax.random.randint(key_list[1], (ALL_PAIRS,), 0, PBLK_DEV), jax.random.fold_in(key_list[1], 1), 0, PBLK_DEV - 1).astype(jnp.int32),
        "pair_atm": draw_pair_atm(jax.random.fold_in(key_list[5], 71), 0),
        "numerators": touch_ends(jax.random.randint(key_list[3], (ALL_PAIRS, PATCH_BLK, CELL_BLK), 0, 16777216), jax.random.fold_in(key_list[3], 1), 0, 16777215).astype(jnp.int32),
        "counts": draw_counts(jax.random.fold_in(key_list[5], 71), 0),
    }


SCALE = 2.0 ** -27


def reference(patches, pair_patch, pair_atm, numerators, counts):
    devices_all = N_BAND * N_TILE
    pairs_here = 2 * PBLK_DEV
    blocks_owned = CELLS_DEV // CELL_BLK
    grouped = patches.reshape(devices_all, PBLK_DEV, PATCH_BLK, FLUX)
    patch_table = pair_patch.reshape(devices_all, pairs_here)
    atm_table = pair_atm.reshape(devices_all, pairs_here)
    numer_table = numerators.reshape(devices_all, pairs_here, PATCH_BLK, CELL_BLK)

    def add_device(accumulated, inputs):
        dev_blocks, patch_index, atm_index, numerator, live_count = inputs
        live_mask = (jnp.arange(pairs_here) < live_count).astype(jnp.float32)
        weight = (numerator.astype(jnp.float32) * SCALE).astype(jnp.bfloat16)
        weight = lax.optimization_barrier(weight).astype(jnp.float32)
        chosen = dev_blocks[patch_index.astype(jnp.int32)].astype(jnp.float32)
        partial_value = jnp.einsum("jpa,jpf->jaf", weight, chosen, precision=lax.Precision.HIGHEST)
        partial_value = partial_value * live_mask[:, None, None]
        return accumulated.at[atm_index.astype(jnp.int32)].add(partial_value), None

    initial = jnp.zeros((devices_all * blocks_owned, CELL_BLK, FLUX), jnp.float32)
    accumulated, unused = lax.scan(add_device, initial, (grouped, patch_table, atm_table, numer_table, counts))
    return accumulated.reshape(devices_all * blocks_owned * CELL_BLK, FLUX)
```

```python
import functools

import jax
import jax.numpy as jnp
from jax import lax
from jax.experimental import pallas as pl
from jax.experimental.pallas import tpu as pltpu
from jax.sharding import PartitionSpec as P

CELLS_DEV = 4096


SCALE = 2.0 ** (-27)
LABEL_ROWS = 8
UNROLL = 16


def shifted(value, axis, steps):
    count = lax.axis_size(axis)
    first, last = (max(0, -steps), min(count, count - steps))
    return lax.ppermute(value, axis, [(source, source + steps) for source in range(first, last)])


def pack_kernel(
    tile_count, blocks_owned, slots,
    place_ref, count_ref, patch_ref, atm_ref, empty_ref, patches_hbm, numer_hbm,
    tile_out, upper_out, lower_out,
    buckets, patches, numer, table, used, row_of, patch_sem, numer_sem, table_sem, out_sem,
):
    pairs_here, cell_rows, patch_rows = numer.shape
    chunks = pairs_here // UNROLL
    bucket_rows = slots * cell_rows + LABEL_ROWS
    table_copy = pltpu.make_async_copy(empty_ref, table, table_sem)
    table_copy.start()
    patch_copy = pltpu.make_async_copy(patches_hbm, patches, patch_sem)
    patch_copy.start()

    def numer_copy(chunk):
        part = pl.ds(pl.multiple_of(chunk * UNROLL, UNROLL), UNROLL)
        return pltpu.make_async_copy(numer_hbm.at[part], numer.at[part], numer_sem.at[chunk])

    for chunk in range(chunks):
        numer_copy(chunk).start()

    count = count_ref[0]
    band_now, tile_now = place_ref[0], place_ref[1]
    del tile_now

    def clear(step, carry):
        rows = pl.ds(pl.multiple_of(step * cell_rows, cell_rows), cell_rows)
        for bucket in range(tile_count + 2):
            buckets[bucket, rows, :] = jnp.zeros((cell_rows, buckets.shape[2]), jnp.float32)
        return carry

    lax.fori_loop(0, slots, clear, 0)
    for bucket in range(tile_count + 2):
        buckets[bucket, pl.ds(slots * cell_rows, LABEL_ROWS), :] = jnp.zeros(
            (LABEL_ROWS, buckets.shape[2]), jnp.float32
        )
        used[bucket] = 0
    used[tile_count + 2] = 0
    table_copy.wait()
    lane = lax.broadcasted_iota(jnp.int32, (1, buckets.shape[2]), 1)

    def place(step, carry):
        for inner in range(4):
            pair = step * 4 + inner
            live = pair < count
            atm = atm_ref[pair]
            owner = lax.div(atm, blocks_owned)
            block = atm - owner * blocks_owned
            owner_band = lax.div(owner, tile_count)
            owner_tile = owner - owner_band * tile_count
            beyond = jnp.where(owner_band > band_now, tile_count, tile_count + 1)
            bucket = jnp.where(owner_band == band_now, owner_tile, beyond)
            bucket = jnp.where(live, bucket, tile_count + 2)
            key = bucket * blocks_owned + block
            known = table[key]
            fresh = known < 0
            slot = jnp.where(fresh, used[bucket], known)
            slot = jnp.where(live, slot, 0)
            table[key] = slot
            used[bucket] = used[bucket] + jnp.where(fresh, 1, 0)
            row_of[pair] = bucket * bucket_rows + slot * cell_rows
            row = pl.ds(slots * cell_rows, 1)
            label = (block + 1).astype(jnp.float32)
            buckets[bucket, row, :] = jnp.where(lane == slot, label, buckets[bucket, row, :])
        return carry

    lax.fori_loop(0, pairs_here // 4, place, 0)
    patch_copy.wait()
    flat = buckets.reshape(buckets.shape[0] * bucket_rows, buckets.shape[2])

    def multiply(chunk, carry):
        numer_copy(chunk).wait()
        results = []
        for inner in range(UNROLL):
            pair = chunk * UNROLL + inner
            weight = (numer[pair].astype(jnp.float32) * SCALE).astype(jnp.bfloat16)
            start = pl.multiple_of(patch_ref[pair] * patch_rows, patch_rows)
            source = patches[pl.ds(start, patch_rows), :]
            results.append(jnp.dot(weight, source, preferred_element_type=jnp.float32))
        for inner in range(UNROLL):
            rows = pl.ds(pl.multiple_of(row_of[chunk * UNROLL + inner], 8), cell_rows)
            flat[rows, :] = flat[rows, :] + results[inner]
        return carry

    busy = lax.div(count + UNROLL - 1, UNROLL)
    lax.fori_loop(0, busy, multiply, 0)

    def drain(chunk, carry):
        numer_copy(chunk).wait()
        return carry

    lax.fori_loop(busy, chunks, drain, 0)
    copies = (
        pltpu.make_async_copy(buckets.at[pl.ds(0, tile_count)], tile_out, out_sem.at[0]),
        pltpu.make_async_copy(buckets.at[tile_count], upper_out, out_sem.at[1]),
        pltpu.make_async_copy(buckets.at[tile_count + 1], lower_out, out_sem.at[2]),
    )
    for copy in copies:
        copy.start()
    for copy in copies:
        copy.wait()


def pack(place, counts, pair_patch, pair_atm, patches, numer, tile_count, blocks_owned, slots):
    pairs_here, cell_rows, patch_rows = numer.shape
    flux_width = patches.shape[1]
    bucket_rows = slots * cell_rows + LABEL_ROWS
    keys = (tile_count + 3) * blocks_owned
    empty = jnp.full((keys,), -1, jnp.int32)
    smem, hbm = pl.BlockSpec(memory_space=pltpu.SMEM), pl.BlockSpec(memory_space=pl.ANY)
    bucket = jax.ShapeDtypeStruct((bucket_rows, flux_width), jnp.float32)
    return pl.pallas_call(
        functools.partial(pack_kernel, tile_count, blocks_owned, slots),
        out_shape=(
            jax.ShapeDtypeStruct((tile_count, bucket_rows, flux_width), jnp.float32), bucket, bucket,
        ),
        in_specs=[smem, smem, smem, smem, hbm, hbm, hbm],
        out_specs=(hbm, hbm, hbm),
        scratch_shapes=[
            pltpu.VMEM((tile_count + 3, bucket_rows, flux_width), jnp.float32),
            pltpu.VMEM(patches.shape, patches.dtype),
            pltpu.VMEM(numer.shape, numer.dtype),
            pltpu.SMEM((keys,), jnp.int32),
            pltpu.SMEM((tile_count + 3,), jnp.int32),
            pltpu.SMEM((pairs_here,), jnp.int32),
            pltpu.SemaphoreType.DMA,
            pltpu.SemaphoreType.DMA((pairs_here // UNROLL,)),
            pltpu.SemaphoreType.DMA,
            pltpu.SemaphoreType.DMA((3,)),
        ],
        name="pack",
    )(place, counts, pair_patch, pair_atm, empty, patches, numer)


def unpack_kernel(
    slots, cell_rows,
    tile_hbm, below_hbm, above_hbm, out_hbm,
    total, buckets, label_rows, labels, in_sem, label_sem, out_sem,
):
    tile_count = tile_hbm.shape[0]
    copies = [
        pltpu.make_async_copy(tile_hbm.at[bucket], buckets.at[bucket], in_sem.at[bucket])
        for bucket in range(tile_count)
    ]
    copies.append(pltpu.make_async_copy(below_hbm, buckets.at[tile_count], in_sem.at[tile_count]))
    copies.append(
        pltpu.make_async_copy(above_hbm, buckets.at[tile_count + 1], in_sem.at[tile_count + 1])
    )
    for copy in copies:
        copy.start()

    def clear(step, carry):
        rows = pl.ds(pl.multiple_of(step * 128, 128), 128)
        total[rows, :] = jnp.zeros((128, total.shape[1]), jnp.float32)
        return carry

    lax.fori_loop(0, total.shape[0] // 128, clear, 0)
    for copy in copies:
        copy.wait()
    for bucket in range(tile_count + 2):
        row = buckets[bucket, pl.ds(slots * cell_rows, 1), :]
        label_rows[pl.ds(bucket, 1), :] = row.astype(jnp.int32) - 1
    label_copy = pltpu.make_async_copy(label_rows, labels, label_sem)
    label_copy.start()
    label_copy.wait()

    def add(bucket, carry):
        for slot in range(slots):
            label = labels[bucket, slot]

            @pl.when(label >= 0)
            def _():
                rows = pl.ds(pl.multiple_of(label * cell_rows, cell_rows), cell_rows)
                total[rows, :] = total[rows, :] + buckets[bucket, pl.ds(slot * cell_rows, cell_rows), :]

        return carry

    lax.fori_loop(0, tile_count + 2, add, 0)
    out_copy = pltpu.make_async_copy(total, out_hbm, out_sem)
    out_copy.start()
    out_copy.wait()


def unpack(tile_in, below, above, blocks_owned, cell_rows, slots):
    tile_count, bucket_rows, flux_width = tile_in.shape
    hbm = pl.BlockSpec(memory_space=pl.ANY)
    total = (blocks_owned * cell_rows, flux_width)
    label_shape = (-(-(tile_count + 2) // 8) * 8, flux_width)
    return pl.pallas_call(
        functools.partial(unpack_kernel, slots, cell_rows),
        out_shape=jax.ShapeDtypeStruct(total, jnp.float32),
        in_specs=[hbm, hbm, hbm],
        out_specs=hbm,
        scratch_shapes=[
            pltpu.VMEM(total, jnp.float32),
            pltpu.VMEM((tile_count + 2, bucket_rows, flux_width), jnp.float32),
            pltpu.VMEM(label_shape, jnp.int32),
            pltpu.SMEM(label_shape, jnp.int32),
            pltpu.SemaphoreType.DMA((tile_count + 2,)),
            pltpu.SemaphoreType.DMA,
            pltpu.SemaphoreType.DMA,
        ],
        name="unpack",
    )(tile_in, below, above)


def per_device(patches, pair_patch, pair_atm, numerators, counts):
    pairs_here, patch_rows, cell_rows = numerators.shape
    blocks_owned = CELLS_DEV // cell_rows
    slots = pairs_here // 8
    tile_count = lax.axis_size("tile")
    place = jnp.stack([lax.axis_index("band"), lax.axis_index("tile")]).astype(jnp.int32)
    numer = jnp.swapaxes(numerators, 1, 2)
    tiles, upper, lower = pack(
        place, counts, pair_patch, pair_atm, patches, numer, tile_count, blocks_owned, slots
    )
    tiles = lax.all_to_all(tiles, "tile", split_axis=0, concat_axis=0, tiled=True)
    below = shifted(upper, "band", 1)
    above = shifted(lower, "band", -1)
    return unpack(tiles, below, above, blocks_owned, cell_rows, slots)


def solution(mesh):
    placed = (
        P(("band", "tile"), None),
        P(("band", "tile")),
        P(("band", "tile")),
        P(("band", "tile"), None, None),
        P(("band", "tile")),
    )
    return jax.shard_map(
        per_device, mesh=mesh, in_specs=placed, out_specs=P(("band", "tile"), None), check_vma=False
    )
```

```python
import functools

import jax
import jax.numpy as jnp
from jax import lax
from jax.experimental import pallas as pl
from jax.experimental.pallas import tpu as pltpu
from jax.sharding import PartitionSpec as P

CELLS_DEV = 4096


SCALE = 2.0 ** (-27)
LABEL_ROWS = 8
UNROLL = 16
VMEM_BYTES = 16 * 2**20
PACK_VMEM = 60 * 1024 * 1024


def shifted(value, axis, steps):
    count = lax.axis_size(axis)
    first, last = (max(0, -steps), min(count, count - steps))
    return lax.ppermute(value, axis, [(source, source + steps) for source in range(first, last)])


def pack_kernel(
    tile_count, blocks_owned, slots, count_hbm, patch_hbm, atm_hbm, patches_hbm, numer_hbm, *rest
):
    outs, rest = rest[: tile_count + 2], rest[tile_count + 2 :]
    count_ref, patch_ref, atm_ref = rest[:3]
    buckets, patches, numer, table, used, row_of, patch_sem, numer_sem, index_sem = rest[3:]
    pairs_here, cell_rows, patch_rows = numer.shape
    chunks = pairs_here // UNROLL
    flux_width = buckets.shape[2]
    bucket_rows = slots * cell_rows + LABEL_ROWS
    index_copies = [
        pltpu.make_async_copy(count_hbm, count_ref, index_sem.at[0]),
        pltpu.make_async_copy(patch_hbm, patch_ref, index_sem.at[1]),
        pltpu.make_async_copy(atm_hbm, atm_ref, index_sem.at[2]),
    ]
    for copy in index_copies:
        copy.start()
    patch_copy = pltpu.make_async_copy(patches_hbm, patches, patch_sem)
    patch_copy.start()

    def numer_copy(chunk):
        part = pl.ds(pl.multiple_of(chunk * UNROLL, UNROLL), UNROLL)
        return pltpu.make_async_copy(numer_hbm.at[part], numer.at[part], numer_sem.at[chunk])

    for chunk in range(chunks):
        numer_copy(chunk).start()

    band_now, tile_now = lax.axis_index("band"), lax.axis_index("tile")

    def clear(step, carry):
        rows = pl.ds(pl.multiple_of(step * cell_rows, cell_rows), cell_rows)
        for bucket in range(tile_count + 2):
            buckets[bucket, rows, :] = jnp.zeros((cell_rows, flux_width), jnp.float32)
        return carry

    lax.fori_loop(0, slots, clear, 0)

    def forget(step, carry):
        for inner in range(16):
            table[step * 16 + inner] = -1
        return carry

    lax.fori_loop(0, (tile_count + 3) * blocks_owned // 16, forget, 0)
    for bucket in range(tile_count + 2):
        buckets[bucket, pl.ds(slots * cell_rows, LABEL_ROWS), :] = jnp.zeros((LABEL_ROWS, flux_width), jnp.float32)
        used[bucket] = 0
    used[tile_count + 2] = 0
    lane = lax.broadcasted_iota(jnp.int32, (1, flux_width), 1)
    for copy in index_copies:
        copy.wait()
    count = count_ref[0]

    def place(step, carry):
        for inner in range(4):
            pair = step * 4 + inner
            live = pair < count
            atm = atm_ref[pair]
            owner = lax.div(atm, blocks_owned)
            block = atm - owner * blocks_owned
            owner_band = lax.div(owner, tile_count)
            owner_tile = owner - owner_band * tile_count
            beyond = jnp.where(owner_band > band_now, tile_count, tile_count + 1)
            bucket = jnp.where(owner_band == band_now, owner_tile ^ tile_now, beyond)
            bucket = jnp.where(live, bucket, tile_count + 2)
            key = bucket * blocks_owned + block
            known = table[key]
            fresh = known < 0
            slot = jnp.where(fresh, used[bucket], known)
            slot = jnp.where(live, slot, 0)
            table[key] = slot
            used[bucket] = used[bucket] + jnp.where(fresh, 1, 0)
            row_of[pair] = bucket * bucket_rows + slot * cell_rows
            row = pl.ds(slots * cell_rows, 1)
            label = (block + 1).astype(jnp.float32)
            buckets[bucket, row, :] = jnp.where(lane == slot, label, buckets[bucket, row, :])
        return carry

    lax.fori_loop(0, pairs_here // 4, place, 0)
    patch_copy.wait()
    flat = buckets.reshape(buckets.shape[0] * bucket_rows, flux_width)

    def multiply(chunk, carry):
        numer_copy(chunk).wait()
        results = []
        for inner in range(UNROLL):
            pair = chunk * UNROLL + inner
            weight = (numer[pair].astype(jnp.float32) * SCALE).astype(jnp.bfloat16)
            start = pl.multiple_of(patch_ref[pair] * patch_rows, patch_rows)
            source = patches[pl.ds(start, patch_rows), :]
            results.append(jnp.dot(weight, source, preferred_element_type=jnp.float32))
        for inner in range(UNROLL):
            rows = pl.ds(pl.multiple_of(row_of[chunk * UNROLL + inner], 8), cell_rows)
            flat[rows, :] = flat[rows, :] + results[inner]
        return carry

    busy = lax.div(count + UNROLL - 1, UNROLL)
    lax.fori_loop(0, busy, multiply, 0)

    def drain(chunk, carry):
        numer_copy(chunk).wait()
        return carry

    lax.fori_loop(busy, chunks, drain, 0)

    def hand_over(step, carry):
        rows = pl.ds(pl.multiple_of(step * cell_rows, cell_rows), cell_rows)
        for bucket, out in enumerate(outs):
            out[rows, :] = buckets[bucket, rows, :]
        return carry

    lax.fori_loop(0, slots, hand_over, 0)
    rows = pl.ds(slots * cell_rows, LABEL_ROWS)
    for bucket, out in enumerate(outs):
        out[rows, :] = buckets[bucket, rows, :]


def pack(counts, pair_patch, pair_atm, patches, numer, tile_count, blocks_owned, slots):
    pairs_here, cell_rows, patch_rows = numer.shape
    flux_width = patches.shape[1]
    bucket_rows = slots * cell_rows + LABEL_ROWS
    keys = (tile_count + 3) * blocks_owned
    hbm, vmem = pl.BlockSpec(memory_space=pltpu.HBM), pl.BlockSpec(memory_space=pltpu.VMEM)
    bucket = jax.ShapeDtypeStruct((bucket_rows, flux_width), jnp.float32)
    return pl.pallas_call(
        functools.partial(pack_kernel, tile_count, blocks_owned, slots),
        out_shape=(bucket,) * (tile_count + 2),
        in_specs=[hbm] * 5,
        out_specs=(vmem,) * (tile_count + 2),
        scratch_shapes=[
            pltpu.SMEM(counts.shape, jnp.int32),
            pltpu.SMEM((pairs_here,), jnp.int32),
            pltpu.SMEM((pairs_here,), jnp.int32),
            pltpu.VMEM((tile_count + 3, bucket_rows, flux_width), jnp.float32),
            pltpu.VMEM(patches.shape, patches.dtype),
            pltpu.VMEM(numer.shape, numer.dtype),
            pltpu.SMEM((keys,), jnp.int32),
            pltpu.SMEM((tile_count + 3,), jnp.int32),
            pltpu.SMEM((pairs_here,), jnp.int32),
            pltpu.SemaphoreType.DMA,
            pltpu.SemaphoreType.DMA((pairs_here // UNROLL,)),
            pltpu.SemaphoreType.DMA((3,)),
        ],
        compiler_params=pltpu.CompilerParams(vmem_limit_bytes=PACK_VMEM),
        name="pack",
    )(counts, pair_patch, pair_atm, patches, numer)


def add_parts(parts, total, label_rows, labels, label_sem, slots, cell_rows):
    for index, part in enumerate(parts):
        row = part[pl.ds(slots * cell_rows, 1), :]
        label_rows[pl.ds(index, 1), :] = row.astype(jnp.int32) - 1
    label_copy = pltpu.make_async_copy(label_rows, labels, label_sem)
    label_copy.start()
    label_copy.wait()
    for index, part in enumerate(parts):
        def add(slot, carry):
            label = labels[index, slot]

            @pl.when(label >= 0)
            def _():
                rows = pl.ds(pl.multiple_of(label * cell_rows, cell_rows), cell_rows)
                here = pl.ds(pl.multiple_of(slot * cell_rows, cell_rows), cell_rows)
                total[rows, :] = total[rows, :] + part[here, :]

            return carry

        lax.fori_loop(0, slots, add, 0)


def first_kernel(count, slots, cell_rows, *rest):
    parts, (total, label_rows, labels, label_sem) = rest[:count], rest[count:]

    def clear(step, carry):
        rows = pl.ds(pl.multiple_of(step * 128, 128), 128)
        total[rows, :] = jnp.zeros((128, total.shape[1]), jnp.float32)
        return carry

    lax.fori_loop(0, total.shape[0] // 128, clear, 0)
    add_parts(parts, total, label_rows, labels, label_sem, slots, cell_rows)


def last_kernel(count, slots, cell_rows, *rest):
    parts, (before, total, out_hbm, label_rows, labels, label_sem, out_sem) = rest[:count], rest[count:]
    del before
    add_parts(parts, total, label_rows, labels, label_sem, slots, cell_rows)
    out_copy = pltpu.make_async_copy(total, out_hbm, out_sem)
    out_copy.start()
    out_copy.wait()


def unpack(parts, before, blocks_owned, cell_rows, slots):
    flux_width = parts[0].shape[1]
    hbm, vmem = pl.BlockSpec(memory_space=pl.ANY), pl.BlockSpec(memory_space=pltpu.VMEM)
    total = jax.ShapeDtypeStruct((blocks_owned * cell_rows, flux_width), jnp.float32)
    label_shape = (-(-len(parts) // 8) * 8, flux_width)
    scratch = [
        pltpu.VMEM(label_shape, jnp.int32),
        pltpu.SMEM(label_shape, jnp.int32),
        pltpu.SemaphoreType.DMA,
    ]
    params = pltpu.CompilerParams(vmem_limit_bytes=VMEM_BYTES)
    if before is None:
        return pl.pallas_call(
            functools.partial(first_kernel, len(parts), slots, cell_rows),
            out_shape=total,
            in_specs=[vmem] * len(parts),
            out_specs=vmem,
            scratch_shapes=scratch,
            compiler_params=params,
            name="unpack_first",
        )(*parts)
    return pl.pallas_call(
        functools.partial(last_kernel, len(parts), slots, cell_rows),
        out_shape=(total, total),
        in_specs=[vmem] * (len(parts) + 1),
        out_specs=(vmem, hbm),
        scratch_shapes=scratch + [pltpu.SemaphoreType.DMA],
        input_output_aliases={len(parts): 0},
        compiler_params=params,
        name="unpack_last",
    )(*parts, before)[1]


def per_device(patches, pair_patch, pair_atm, numerators, counts):
    pairs_here, patch_rows, cell_rows = numerators.shape
    blocks_owned = CELLS_DEV // cell_rows
    slots = pairs_here // 8
    tile_count = lax.axis_size("tile")
    numer = jnp.swapaxes(numerators, 1, 2)
    own, *parts = pack(counts, pair_patch, pair_atm, patches, numer, tile_count, blocks_owned, slots)
    received = {}
    for mask in reversed(range(1, tile_count)):
        pairs = [(tile, tile ^ mask) for tile in range(tile_count)]
        received[mask] = lax.ppermute(parts[mask - 1], "tile", pairs)
    bands = [shifted(parts[tile_count - 1], "band", 1), shifted(parts[tile_count], "band", -1)]
    half = tile_count // 2
    early = [own, *bands] + [received[mask] for mask in range(1, half)]
    total = unpack(early, None, blocks_owned, cell_rows, slots)
    late = [received[mask] for mask in range(half, tile_count)]
    return unpack(late, total, blocks_owned, cell_rows, slots)


def solution(mesh):
    placed = (
        P(("band", "tile"), None),
        P(("band", "tile")),
        P(("band", "tile")),
        P(("band", "tile"), None, None),
        P(("band", "tile")),
    )
    return jax.shard_map(
        per_device, mesh=mesh, in_specs=placed, out_specs=P(("band", "tile"), None), check_vma=False
    )
```

```python
import functools

import jax
import jax.numpy as jnp
from jax import lax
from jax.experimental import pallas as pl
from jax.experimental.pallas import tpu as pltpu
from jax.sharding import PartitionSpec as P

CELLS_DEV = 4096


SCALE = 2.0 ** (-27)
LABEL_ROWS = 8
UNROLL = 32
VMEM_BYTES = 16 * 2**20
PACK_VMEM = 50 * 2**20


def shifted(value, axis, steps):
    count = lax.axis_size(axis)
    first, last = (max(0, -steps), min(count, count - steps))
    return lax.ppermute(value, axis, [(source, source + steps) for source in range(first, last)])


def pack_kernel(
    tile_count, blocks_owned, slots, index_in, patches_hbm, numer_hbm, *rest
):
    outs, rest = rest[: tile_count + 2], rest[tile_count + 2 :]
    index, buckets, patches, numer, table, used, row_of, patch_sem, numer_sem, index_sem = rest
    pairs_here, cell_rows, patch_rows = numer.shape
    chunks = pairs_here // UNROLL
    flux_width = buckets.shape[2]
    bucket_rows = slots * cell_rows + LABEL_ROWS
    index_copy = pltpu.make_async_copy(index_in, index, index_sem)
    index_copy.start()
    patch_copy = pltpu.make_async_copy(patches_hbm, patches, patch_sem)
    patch_copy.start()

    def numer_copy(chunk):
        part = pl.ds(pl.multiple_of(chunk * UNROLL, UNROLL), UNROLL)
        return pltpu.make_async_copy(numer_hbm.at[part], numer.at[part], numer_sem.at[chunk])

    for chunk in range(chunks):
        numer_copy(chunk).start()

    band_now, tile_now = lax.axis_index("band"), lax.axis_index("tile")

    def clear(step, carry):
        rows = pl.ds(pl.multiple_of(step * cell_rows, cell_rows), cell_rows)
        for bucket in range(tile_count + 2):
            buckets[bucket, rows, :] = jnp.zeros((cell_rows, flux_width), jnp.float32)
        return carry

    lax.fori_loop(0, slots, clear, 0)

    def forget(step, carry):
        for inner in range(16):
            table[step * 16 + inner] = -1
        return carry

    lax.fori_loop(0, (tile_count + 3) * blocks_owned // 16, forget, 0)
    for bucket in range(tile_count + 2):
        buckets[bucket, pl.ds(slots * cell_rows, LABEL_ROWS), :] = jnp.zeros((LABEL_ROWS, flux_width), jnp.float32)
        used[bucket] = 0
    used[tile_count + 2] = 0
    lane = lax.broadcasted_iota(jnp.int32, (1, flux_width), 1)
    index_copy.wait()
    count = index[2, 0]

    def place(step, carry):
        for inner in range(4):
            pair = step * 4 + inner
            live = pair < count
            atm = index[1, pair]
            owner = lax.div(atm, blocks_owned)
            block = atm - owner * blocks_owned
            owner_band = lax.div(owner, tile_count)
            owner_tile = owner - owner_band * tile_count
            beyond = jnp.where(owner_band > band_now, tile_count, tile_count + 1)
            bucket = jnp.where(owner_band == band_now, owner_tile ^ tile_now, beyond)
            bucket = jnp.where(live, bucket, tile_count + 2)
            key = bucket * blocks_owned + block
            known = table[key]
            fresh = known < 0
            slot = jnp.where(fresh, used[bucket], known)
            slot = jnp.where(live, slot, 0)
            table[key] = slot
            used[bucket] = used[bucket] + jnp.where(fresh, 1, 0)
            row_of[pair] = bucket * bucket_rows + slot * cell_rows
            row = pl.ds(slots * cell_rows, 1)
            label = (block + 1).astype(jnp.float32)
            buckets[bucket, row, :] = jnp.where(lane == slot, label, buckets[bucket, row, :])
        return carry

    lax.fori_loop(0, pairs_here // 4, place, 0)
    patch_copy.wait()
    flat = buckets.reshape(buckets.shape[0] * bucket_rows, flux_width)

    def multiply(chunk, carry):
        numer_copy(chunk).wait()
        results = []
        for inner in range(UNROLL):
            pair = chunk * UNROLL + inner
            weight = (numer[pair].astype(jnp.float32) * SCALE).astype(jnp.bfloat16)
            start = pl.multiple_of(index[0, pair] * patch_rows, patch_rows)
            source = patches[pl.ds(start, patch_rows), :]
            results.append(jnp.dot(weight, source, preferred_element_type=jnp.float32))
        for inner in range(UNROLL):
            rows = pl.ds(pl.multiple_of(row_of[chunk * UNROLL + inner], 8), cell_rows)
            flat[rows, :] = flat[rows, :] + results[inner]
        return carry

    busy = lax.div(count + UNROLL - 1, UNROLL)
    lax.fori_loop(0, busy, multiply, 0)

    def drain(chunk, carry):
        numer_copy(chunk).wait()
        return carry

    lax.fori_loop(busy, chunks, drain, 0)

    def hand_over(step, carry):
        rows = pl.ds(pl.multiple_of(step * cell_rows, cell_rows), cell_rows)
        for bucket, out in enumerate(outs):
            out[rows, :] = buckets[bucket, rows, :]
        return carry

    lax.fori_loop(0, slots, hand_over, 0)
    rows = pl.ds(slots * cell_rows, LABEL_ROWS)
    for bucket, out in enumerate(outs):
        out[rows, :] = buckets[bucket, rows, :]


def pack(counts, pair_patch, pair_atm, patches, numer, tile_count, blocks_owned, slots):
    pairs_here, cell_rows, patch_rows = numer.shape
    flux_width = patches.shape[1]
    bucket_rows = slots * cell_rows + LABEL_ROWS
    keys = (tile_count + 3) * blocks_owned
    hbm, vmem = pl.BlockSpec(memory_space=pltpu.HBM), pl.BlockSpec(memory_space=pltpu.VMEM)
    index = jnp.stack([pair_patch, pair_atm, jnp.broadcast_to(counts, pair_patch.shape)])
    bucket = jax.ShapeDtypeStruct((bucket_rows, flux_width), jnp.float32)
    return pl.pallas_call(
        functools.partial(pack_kernel, tile_count, blocks_owned, slots),
        out_shape=(bucket,) * (tile_count + 2),
        in_specs=[vmem, hbm, hbm],
        out_specs=(vmem,) * (tile_count + 2),
        scratch_shapes=[
            pltpu.SMEM(index.shape, jnp.int32),
            pltpu.VMEM((tile_count + 3, bucket_rows, flux_width), jnp.float32),
            pltpu.VMEM(patches.shape, patches.dtype),
            pltpu.VMEM(numer.shape, numer.dtype),
            pltpu.SMEM((keys,), jnp.int32),
            pltpu.SMEM((tile_count + 3,), jnp.int32),
            pltpu.SMEM((pairs_here,), jnp.int32),
            pltpu.SemaphoreType.DMA,
            pltpu.SemaphoreType.DMA((pairs_here // UNROLL,)),
            pltpu.SemaphoreType.DMA,
        ],
        compiler_params=pltpu.CompilerParams(vmem_limit_bytes=PACK_VMEM),
        name="pack",
    )(index, patches, numer)


def add_parts(parts, total, label_rows, labels, label_sem, slots, cell_rows):
    for index, part in enumerate(parts):
        row = part[pl.ds(slots * cell_rows, 1), :]
        label_rows[pl.ds(index, 1), :] = row.astype(jnp.int32) - 1
    label_copy = pltpu.make_async_copy(label_rows, labels, label_sem)
    label_copy.start()
    label_copy.wait()
    for index, part in enumerate(parts):
        def add(slot, carry):
            label = labels[index, slot]

            @pl.when(label >= 0)
            def _():
                rows = pl.ds(pl.multiple_of(label * cell_rows, cell_rows), cell_rows)
                here = pl.ds(pl.multiple_of(slot * cell_rows, cell_rows), cell_rows)
                total[rows, :] = total[rows, :] + part[here, :]

            return carry

        lax.fori_loop(0, slots, add, 0)


def first_kernel(count, slots, cell_rows, *rest):
    parts, (total, label_rows, labels, label_sem) = rest[:count], rest[count:]

    def clear(step, carry):
        rows = pl.ds(pl.multiple_of(step * 128, 128), 128)
        total[rows, :] = jnp.zeros((128, total.shape[1]), jnp.float32)
        return carry

    lax.fori_loop(0, total.shape[0] // 128, clear, 0)
    add_parts(parts, total, label_rows, labels, label_sem, slots, cell_rows)


def last_kernel(count, slots, cell_rows, *rest):
    parts, (before, total, out_hbm, label_rows, labels, label_sem, out_sem) = rest[:count], rest[count:]
    del before
    add_parts(parts, total, label_rows, labels, label_sem, slots, cell_rows)
    out_copy = pltpu.make_async_copy(total, out_hbm, out_sem)
    out_copy.start()
    out_copy.wait()


def unpack(parts, before, blocks_owned, cell_rows, slots):
    flux_width = parts[0].shape[1]
    hbm, vmem = pl.BlockSpec(memory_space=pl.ANY), pl.BlockSpec(memory_space=pltpu.VMEM)
    total = jax.ShapeDtypeStruct((blocks_owned * cell_rows, flux_width), jnp.float32)
    label_shape = (-(-len(parts) // 8) * 8, flux_width)
    scratch = [
        pltpu.VMEM(label_shape, jnp.int32),
        pltpu.SMEM(label_shape, jnp.int32),
        pltpu.SemaphoreType.DMA,
    ]
    params = pltpu.CompilerParams(vmem_limit_bytes=VMEM_BYTES)
    if before is None:
        return pl.pallas_call(
            functools.partial(first_kernel, len(parts), slots, cell_rows),
            out_shape=total,
            in_specs=[vmem] * len(parts),
            out_specs=vmem,
            scratch_shapes=scratch,
            compiler_params=params,
            name="unpack_first",
        )(*parts)
    return pl.pallas_call(
        functools.partial(last_kernel, len(parts), slots, cell_rows),
        out_shape=(total, total),
        in_specs=[vmem] * (len(parts) + 1),
        out_specs=(vmem, hbm),
        scratch_shapes=scratch + [pltpu.SemaphoreType.DMA],
        input_output_aliases={len(parts): 0},
        compiler_params=params,
        name="unpack_last",
    )(*parts, before)[1]


def per_device(patches, pair_patch, pair_atm, numerators, counts):
    pairs_here, patch_rows, cell_rows = numerators.shape
    blocks_owned = CELLS_DEV // cell_rows
    slots = pairs_here // 8
    tile_count = lax.axis_size("tile")
    numer = jnp.swapaxes(numerators, 1, 2)
    own, *parts = pack(counts, pair_patch, pair_atm, patches, numer, tile_count, blocks_owned, slots)
    received = {}
    for mask in reversed(range(1, tile_count)):
        pairs = [(tile, tile ^ mask) for tile in range(tile_count)]
        received[mask] = lax.ppermute(parts[mask - 1], "tile", pairs)
    bands = [shifted(parts[tile_count - 1], "band", 1), shifted(parts[tile_count], "band", -1)]
    half = tile_count // 2
    early = [own, *bands] + [received[mask] for mask in range(1, half)]
    total = unpack(early, None, blocks_owned, cell_rows, slots)
    late = [received[mask] for mask in range(half, tile_count)]
    return unpack(late, total, blocks_owned, cell_rows, slots)


def solution(mesh):
    placed = (
        P(("band", "tile"), None),
        P(("band", "tile")),
        P(("band", "tile")),
        P(("band", "tile"), None, None),
        P(("band", "tile")),
    )
    return jax.shard_map(
        per_device, mesh=mesh, in_specs=placed, out_specs=P(("band", "tile"), None), check_vma=False
    )
```

```python
import functools

import jax
import jax.numpy as jnp
from jax import lax
from jax.experimental import pallas as pl
from jax.experimental.pallas import tpu as pltpu
from jax.sharding import PartitionSpec as P


CELLS_DEV = 4096


SCALE = 2.0 ** (-27)
LABEL_ROWS = 8
UNROLL = 32
LEAD_UNROLL = 16
PACK_VMEM = 50 * 2**20
LEAD_VMEM = 53 * 2**20
ADD_VMEM = 16 * 2**20
HBM = pl.BlockSpec(memory_space=pltpu.HBM)
VMEM = pl.BlockSpec(memory_space=pltpu.VMEM)


def shifted(value, axis, steps):
    count = lax.axis_size(axis)
    first, last = (max(0, -steps), min(count, count - steps))
    return lax.ppermute(value, axis, [(source, source + steps) for source in range(first, last)])


def exchanged(value, mask, tile_count):
    return lax.ppermute(value, "tile", [(tile, tile ^ mask) for tile in range(tile_count)])


def weigh(numer, source):
    weight = (numer.astype(jnp.float32) * SCALE).astype(jnp.bfloat16)
    return jnp.dot(weight, source, preferred_element_type=jnp.float32)


def set_label(bucket, label_row, slot, block):
    lane = lax.broadcasted_iota(jnp.int32, (1, bucket.shape[1]), 1)
    row = pl.ds(label_row, 1)
    bucket[row, :] = jnp.where(lane == slot, (block + 1).astype(jnp.float32), bucket[row, :])


def lead_kernel(
    tile_count, blocks_owned, slots, index_in, patches_hbm, numer_hbm, out,
    found, index, rows, sources, numer, table, used, chosen, slot_of, index_sem, source_sem, numer_sem,
):
    pairs_here, cell_rows, patch_rows = numer_hbm.shape
    locate(index_in, found, blocks_owned, tile_count)
    index_copy = pltpu.make_async_copy(found, index, index_sem)
    index_copy.start()
    most = 2 * slots
    _, flux_width = out.shape

    def clear(step, carry):
        part = pl.ds(pl.multiple_of(step * cell_rows, cell_rows), cell_rows)
        rows[part, :] = jnp.zeros((cell_rows, flux_width), jnp.float32)
        return carry

    lax.fori_loop(0, slots, clear, 0)
    rows[pl.ds(slots * cell_rows, LABEL_ROWS), :] = jnp.zeros((LABEL_ROWS, flux_width), jnp.float32)

    def forget(step, carry):
        for inner in range(16):
            table[step * 16 + inner] = -1
        return carry

    lax.fori_loop(0, blocks_owned // 16, forget, 0)
    for place in range(most):
        slot_of[place] = slots * cell_rows + LABEL_ROWS
    used[0] = 0
    index_copy.wait()

    def copies(pair, place):
        start = pl.multiple_of(index[0, pair] * patch_rows, patch_rows)
        source = pltpu.make_async_copy(
            patches_hbm.at[pl.ds(start, patch_rows)], sources.at[place], source_sem.at[place]
        )
        return source, pltpu.make_async_copy(numer_hbm.at[pair], numer.at[place], numer_sem.at[place])

    def find(step, count):
        for inner in range(8):
            pair = step * 8 + inner
            mine = index[2, pair] == tile_count - 1

            @pl.when(mine)
            def _(pair=pair, count=count):
                for copy in copies(pair, count):
                    copy.start()
                chosen[count] = pair

            count = count + jnp.where(mine, 1, 0)
        return count

    count = lax.fori_loop(0, pairs_here // 8, find, 0)

    def place_pair(place, carry):
        block = index[1, chosen[place]]
        known = table[block]
        fresh = known < 0
        slot = jnp.where(fresh, used[0], known)
        table[block] = slot
        used[0] = used[0] + jnp.where(fresh, 1, 0)
        slot_of[place] = slot * cell_rows
        set_label(rows, slots * cell_rows, slot, block)
        return carry

    lax.fori_loop(0, count, place_pair, 0)

    def wait(place, carry):
        for copy in copies(chosen[place], place):
            copy.wait()
        return carry

    lax.fori_loop(0, count, wait, 0)

    def multiply(step, carry):
        results = [
            weigh(numer[step * LEAD_UNROLL + inner], sources[step * LEAD_UNROLL + inner])
            for inner in range(LEAD_UNROLL)
        ]
        for inner in range(LEAD_UNROLL):
            part = pl.ds(pl.multiple_of(slot_of[step * LEAD_UNROLL + inner], 8), cell_rows)
            rows[part, :] = rows[part, :] + results[inner]
        return carry

    lax.fori_loop(0, lax.div(count + LEAD_UNROLL - 1, LEAD_UNROLL), multiply, 0)
    for slot in range(slots):
        part = pl.ds(slot * cell_rows, cell_rows)
        out[part, :] = rows[part, :]
    part = pl.ds(slots * cell_rows, LABEL_ROWS)
    out[part, :] = rows[part, :]


def lead_bucket(index, patches, numer, tile_count, blocks_owned, slots):
    pairs_here, cell_rows, patch_rows = numer.shape
    flux_width = patches.shape[1]
    bucket_rows = slots * cell_rows + LABEL_ROWS
    most = 2 * slots
    return pl.pallas_call(
        functools.partial(lead_kernel, tile_count, blocks_owned, slots),
        out_shape=jax.ShapeDtypeStruct((bucket_rows, flux_width), jnp.float32),
        in_specs=[VMEM, HBM, HBM],
        out_specs=VMEM,
        scratch_shapes=[
            pltpu.VMEM((4, pairs_here), jnp.int32),
            pltpu.SMEM((4, pairs_here), jnp.int32),
            pltpu.VMEM((bucket_rows + cell_rows, flux_width), jnp.float32),
            pltpu.VMEM((most, patch_rows, flux_width), patches.dtype),
            pltpu.VMEM((most, cell_rows, patch_rows), numer.dtype),
            pltpu.SMEM((blocks_owned,), jnp.int32),
            pltpu.SMEM((1,), jnp.int32),
            pltpu.SMEM((most,), jnp.int32),
            pltpu.SMEM((most,), jnp.int32),
            pltpu.SemaphoreType.DMA,
            pltpu.SemaphoreType.DMA((most,)),
            pltpu.SemaphoreType.DMA((most,)),
        ],
        compiler_params=pltpu.CompilerParams(vmem_limit_bytes=LEAD_VMEM),
        name="lead",
    )(index, patches, numer)


def pack_kernel(tile_count, blocks_owned, slots, index_in, patches_hbm, numer_hbm, *rest):
    places = [place for place in range(tile_count + 2) if place != tile_count - 1]
    outs, rest = rest[: len(places)], rest[len(places) :]
    found, index, buckets, patches, numer, table, used, row_of, patch_sem, numer_sem, index_sem = rest
    pairs_here, cell_rows, patch_rows = numer.shape
    chunks = pairs_here // UNROLL
    flux_width = buckets.shape[2]
    bucket_rows = slots * cell_rows + LABEL_ROWS
    locate(index_in, found, blocks_owned, tile_count)
    index_copy = pltpu.make_async_copy(found, index, index_sem)
    index_copy.start()
    patch_copy = pltpu.make_async_copy(patches_hbm, patches, patch_sem)
    patch_copy.start()

    def numer_copy(chunk):
        part = pl.ds(pl.multiple_of(chunk * UNROLL, UNROLL), UNROLL)
        return pltpu.make_async_copy(numer_hbm.at[part], numer.at[part], numer_sem.at[chunk])

    for chunk in range(chunks):
        numer_copy(chunk).start()

    def clear(step, carry):
        rows = pl.ds(pl.multiple_of(step * cell_rows, cell_rows), cell_rows)
        for bucket in places:
            buckets[bucket, rows, :] = jnp.zeros((cell_rows, flux_width), jnp.float32)
        return carry

    lax.fori_loop(0, slots, clear, 0)

    def forget(step, carry):
        for inner in range(16):
            table[step * 16 + inner] = -1
        return carry

    lax.fori_loop(0, (tile_count + 3) * blocks_owned // 16, forget, 0)
    for bucket in range(tile_count + 3):
        buckets[bucket, pl.ds(slots * cell_rows, LABEL_ROWS), :] = jnp.zeros((LABEL_ROWS, flux_width), jnp.float32)
        used[bucket] = 0
    index_copy.wait()
    count = index[3, 0]

    def place(step, carry):
        for inner in range(4):
            pair = step * 4 + inner
            block, bucket = index[1, pair], index[2, pair]
            here = (bucket != tile_count - 1) & (bucket != tile_count + 2)
            bucket = jnp.where(here, bucket, tile_count + 2)
            key = bucket * blocks_owned + block
            known = table[key]
            fresh = known < 0
            slot = jnp.where(fresh, used[bucket], known)
            slot = jnp.where(here, slot, 0)
            table[key] = slot
            used[bucket] = used[bucket] + jnp.where(fresh, 1, 0)
            row_of[pair] = bucket * bucket_rows + slot * cell_rows
            set_label(buckets.at[bucket], slots * cell_rows, slot, block)
        return carry

    lax.fori_loop(0, pairs_here // 4, place, 0)
    patch_copy.wait()
    flat = buckets.reshape(buckets.shape[0] * bucket_rows, flux_width)

    def multiply(chunk, carry):
        numer_copy(chunk).wait()
        results = []
        for inner in range(UNROLL):
            pair = chunk * UNROLL + inner
            start = pl.multiple_of(index[0, pair] * patch_rows, patch_rows)
            results.append(weigh(numer[pair], patches[pl.ds(start, patch_rows), :]))
        for inner in range(UNROLL):
            rows = pl.ds(pl.multiple_of(row_of[chunk * UNROLL + inner], 8), cell_rows)
            flat[rows, :] = flat[rows, :] + results[inner]
        return carry

    busy = lax.div(count + UNROLL - 1, UNROLL)
    lax.fori_loop(0, busy, multiply, 0)

    def drain(chunk, carry):
        numer_copy(chunk).wait()
        return carry

    lax.fori_loop(busy, chunks, drain, 0)

    def hand_over(step, carry):
        rows = pl.ds(pl.multiple_of(step * cell_rows, cell_rows), cell_rows)
        for bucket, out in zip(places, outs):
            out[rows, :] = buckets[bucket, rows, :]
        return carry

    lax.fori_loop(0, slots, hand_over, 0)
    rows = pl.ds(slots * cell_rows, LABEL_ROWS)
    for bucket, out in zip(places, outs):
        out[rows, :] = buckets[bucket, rows, :]


def pack(index, patches, numer, tile_count, blocks_owned, slots):
    pairs_here, cell_rows, _ = numer.shape
    flux_width = patches.shape[1]
    bucket_rows = slots * cell_rows + LABEL_ROWS
    keys = (tile_count + 3) * blocks_owned
    bucket = jax.ShapeDtypeStruct((bucket_rows, flux_width), jnp.float32)
    return pl.pallas_call(
        functools.partial(pack_kernel, tile_count, blocks_owned, slots),
        out_shape=(bucket,) * (tile_count + 1),
        in_specs=[VMEM, HBM, HBM],
        out_specs=(VMEM,) * (tile_count + 1),
        scratch_shapes=[
            pltpu.VMEM((4, pairs_here), jnp.int32),
            pltpu.SMEM((4, pairs_here), jnp.int32),
            pltpu.VMEM((tile_count + 3, bucket_rows, flux_width), jnp.float32),
            pltpu.VMEM(patches.shape, patches.dtype),
            pltpu.VMEM(numer.shape, numer.dtype),
            pltpu.SMEM((keys,), jnp.int32),
            pltpu.SMEM((tile_count + 3,), jnp.int32),
            pltpu.SMEM((pairs_here,), jnp.int32),
            pltpu.SemaphoreType.DMA,
            pltpu.SemaphoreType.DMA((pairs_here // UNROLL,)),
            pltpu.SemaphoreType.DMA,
        ],
        compiler_params=pltpu.CompilerParams(vmem_limit_bytes=PACK_VMEM),
        name="pack",
    )(index, patches, numer)


def add_parts(parts, total, label_rows, labels, label_sem, slots, cell_rows):
    for number, part in enumerate(parts):
        row = part[pl.ds(slots * cell_rows, 1), :]
        label_rows[pl.ds(number, 1), :] = row.astype(jnp.int32) - 1
    label_copy = pltpu.make_async_copy(label_rows, labels, label_sem)
    label_copy.start()
    label_copy.wait()
    for number, part in enumerate(parts):

        def add(slot, number=number, part=part):
            rows = pl.ds(pl.multiple_of(labels[number, slot] * cell_rows, cell_rows), cell_rows)
            here = pl.ds(pl.multiple_of(slot * cell_rows, cell_rows), cell_rows)
            total[rows, :] = total[rows, :] + part[here, :]
            return slot + 1

        lax.while_loop(lambda slot, number=number: labels[number, slot] >= 0, add, 0)


def first_kernel(count, slots, cell_rows, *rest):
    parts, (total, out_hbm, label_rows, labels, label_sem, out_sem) = rest[:count], rest[count:]

    def clear(step, carry):
        rows = pl.ds(pl.multiple_of(step * 128, 128), 128)
        total[rows, :] = jnp.zeros((128, total.shape[1]), jnp.float32)
        return carry

    lax.fori_loop(0, total.shape[0] // 128, clear, 0)
    add_parts(parts, total, label_rows, labels, label_sem, slots, cell_rows)
    out_copy = pltpu.make_async_copy(total, out_hbm, out_sem)
    out_copy.start()
    out_copy.wait()


def last_kernel(count, slots, cell_rows, *rest):
    parts, (before, early, total, out_hbm, label_rows, labels, label_sem, out_sem) = rest[:count], rest[count:]
    del before, early
    add_parts(parts, total, label_rows, labels, label_sem, slots, cell_rows)

    def copy(number, slot):
        rows = pl.ds(pl.multiple_of(labels[number, slot] * cell_rows, cell_rows), cell_rows)
        return pltpu.make_async_copy(total.at[rows], out_hbm.at[rows], out_sem.at[number, slot])

    for number in range(count):

        def start(slot, number=number):
            copy(number, slot).start()
            return slot + 1

        lax.while_loop(lambda slot, number=number: labels[number, slot] >= 0, start, 0)
    for number in range(count):

        def wait(slot, number=number):
            copy(number, slot).wait()
            return slot + 1

        lax.while_loop(lambda slot, number=number: labels[number, slot] >= 0, wait, 0)


def unpack(parts, before, blocks_owned, cell_rows, slots):
    flux_width = parts[0].shape[1]
    total = jax.ShapeDtypeStruct((blocks_owned * cell_rows, flux_width), jnp.float32)
    label_shape = (-(-len(parts) // 8) * 8, flux_width)
    scratch = [
        pltpu.VMEM(label_shape, jnp.int32),
        pltpu.SMEM(label_shape, jnp.int32),
        pltpu.SemaphoreType.DMA,
    ]
    params = pltpu.CompilerParams(vmem_limit_bytes=ADD_VMEM)
    if before is None:
        return pl.pallas_call(
            functools.partial(first_kernel, len(parts), slots, cell_rows),
            out_shape=(total, total),
            in_specs=[VMEM] * len(parts),
            out_specs=(VMEM, HBM),
            scratch_shapes=scratch + [pltpu.SemaphoreType.DMA],
            compiler_params=params,
            name="unpack_first",
        )(*parts)
    return pl.pallas_call(
        functools.partial(last_kernel, len(parts), slots, cell_rows),
        out_shape=(total, total),
        in_specs=[VMEM] * (len(parts) + 1) + [HBM],
        out_specs=(VMEM, HBM),
        scratch_shapes=scratch + [pltpu.SemaphoreType.DMA((len(parts), slots))],
        input_output_aliases={len(parts): 0, len(parts) + 1: 1},
        compiler_params=params,
        name="unpack_last",
    )(*parts, *before)


def locate(index_in, scratch, blocks_owned, tile_count):
    atm = index_in[pl.ds(1, 1), :]
    lane = lax.broadcasted_iota(jnp.int32, atm.shape, 1)
    owner = lax.div(atm, blocks_owned)
    band = lax.div(owner, tile_count)
    tile = owner - band * tile_count
    band_now = lax.axis_index("band")
    beyond = jnp.where(band > band_now, tile_count, tile_count + 1)
    bucket = jnp.where(band == band_now, tile ^ lax.axis_index("tile"), beyond)
    scratch[pl.ds(0, 1), :] = index_in[pl.ds(0, 1), :]
    scratch[pl.ds(1, 1), :] = atm - owner * blocks_owned
    scratch[pl.ds(2, 1), :] = jnp.where(lane < index_in[pl.ds(2, 1), :], bucket, tile_count + 2)
    scratch[pl.ds(3, 1), :] = index_in[pl.ds(2, 1), :]


def per_device(patches, pair_patch, pair_atm, numerators, counts):
    pairs_here, _, cell_rows = numerators.shape
    blocks_owned = CELLS_DEV // cell_rows
    slots = pairs_here // 8
    tile_count = lax.axis_size("tile")
    numer = jnp.swapaxes(numerators, 1, 2)
    index = jnp.stack([pair_patch, pair_atm, jnp.broadcast_to(counts, pair_patch.shape)])
    sizes = (tile_count, blocks_owned, slots)
    lead = lead_bucket(index, patches, numer, *sizes)
    own, *parts = pack(index, patches, numer, *sizes)
    received = {}
    for mask in reversed(range(1, tile_count)):
        part = lead if mask == tile_count - 1 else parts[mask - 1]
        received[mask] = exchanged(part, mask, tile_count)
    below = shifted(parts[tile_count - 2], "band", 1)
    above = shifted(parts[tile_count - 1], "band", -1)
    half = tile_count // 2
    last = [half, half + 1]
    middle = [mask for mask in range(2, tile_count - 1) if mask not in last]
    stages = (
        [own, received[1], received[tile_count - 1]],
        [below, above] + [received[mask] for mask in middle],
        [received[half + 1]],
        [received[half]],
    )
    totals = None
    for parts in stages:
        totals = unpack(parts, totals, blocks_owned, cell_rows, slots)
    return totals[1]


def solution(mesh):
    placed = (
        P(("band", "tile"), None),
        P(("band", "tile")),
        P(("band", "tile")),
        P(("band", "tile"), None, None),
        P(("band", "tile")),
    )
    return jax.shard_map(
        per_device, mesh=mesh, in_specs=placed, out_specs=P(("band", "tile"), None), check_vma=False
    )
```
